512 devices in a mesh: ctx: 32 (over y, x_lo, core), head: 16 (over z, x_hi).
Axes of the slice: x: 4 (x_hi: 2, x_lo: 2; x = x_hi * 2 + x_lo), y: 8, z: 8, core: 2. Of those that a mesh axis runs over, the one named last changes fastest.
Arguments:
- query_in: bfloat16 [4096, 4096], P(('ctx', 'head')), may hold values from -20 to 20
- key_in: bfloat16 [4096, 4096], P('ctx', 'head'), may hold values from -20 to 20
- value_in: bfloat16 [4096, 4096], P('ctx', 'head'), may hold values from -6 to 6
- out_saved: bfloat16 [4096, 4096], P(('ctx', 'head')), may hold values from -1.5 to 1.5
- out_grad: bfloat16 [4096, 4096], P(('ctx', 'head')), may hold values from -24 to 24
- span_place: int32 [64], replicated, may hold values from 0 to 63, each once
Outputs:
- grad_query: bfloat16 [4096, 4096], P(('ctx', 'head'))
- grad_key: bfloat16 [4096, 4096], P('ctx', 'head')
- grad_value: bfloat16 [4096, 4096], P('ctx', 'head')
The draws below stay inside these ranges and needn't reach their ends.
Inputs may be any that keep to these rules, and one draw needn't show every extreme that they name: `span_place`: each block position appears once.
All inputs are finite; a program needn't handle non-finite values.
Results may differ from the reference program's by a relative error of at most 0.0049.
Values may be sent and summed in bfloat16 or wider, within the bound.
No kernel may reach another device: no remote copies, remote signals or barrier semaphores. Data moves between devices by JAX's collectives and lax.ppermute only.
A program may use at most 64 MiB of HBM per device.

```python
import jax
import jax.numpy as jnp
from jax import lax

HEAD_DIM = 128
HEADS = 32
SPAN = 64
SPANS = 64
SEQUENCE_TOKENS = 4096


def drawn_pair(key):
    root_random_key = jax.random.fold_in(key, 4242)
    random_key_for_queries, random_key_for_keys = jax.random.split(root_random_key, 2)
    shape = (SEQUENCE_TOKENS, HEADS * HEAD_DIM)
    queries = jnp.clip(jax.random.normal(random_key_for_queries, shape, jnp.float32), -6.0, 6.0)
    keyset = jnp.clip(jax.random.normal(random_key_for_keys, shape, jnp.float32), -6.0, 6.0)
    return (queries, keyset)


def draw_query_in(key, part):
    return drawn_pair(key)[0].astype(jnp.bfloat16)


def draw_key_in(key, part):
    return drawn_pair(key)[1].astype(jnp.bfloat16)


def shard_levels(stream_key, dims, cuts, low, top_value):
    level, own = 1.0, jax.random.fold_in(stream_key, 6)
    for dim, blocks in cuts:
        heights = jnp.exp(jax.random.uniform(jax.random.fold_in(own, dim), (blocks,), jnp.float32, low / len(cuts), top_value / len(cuts)))
        level = level * jnp.repeat(heights, dims[dim] // blocks).reshape([-1 if axis == dim else 1 for axis in range(len(dims))])
    return level


def centred(rng, shape, width, bound, cuts=(), kind=jnp.bfloat16):
    entries = width * jax.random.normal(rng, shape, jnp.float32)
    if cuts:
        entries = entries * shard_levels(rng, shape, cuts, -0.22, 0.18)
    return jnp.clip(entries, -bound, bound).astype(kind)


def setup_inputs(seed: int = 0) -> dict:
    streams_of = jax.random.split(jax.random.key(seed), 7)
    query_in = draw_query_in(jax.random.fold_in(streams_of[6], 71), 0)
    key_in = draw_key_in(jax.random.fold_in(streams_of[6], 71), 0)
    value_in = centred(streams_of[2], (SEQUENCE_TOKENS, HEADS * HEAD_DIM), 1.0, 6.0, ((0, 32), (1, 16)))
    out_saved = centred(streams_of[3], (SEQUENCE_TOKENS, HEADS * HEAD_DIM), 0.25, 1.5, ((0, 512),))
    out_grad = centred(streams_of[4], (SEQUENCE_TOKENS, HEADS * HEAD_DIM), 4.0, 24.0, ((0, 512),))
    span_place = jax.random.permutation(streams_of[5], SPANS).astype(jnp.int32)
    return {"query_in": query_in, "key_in": key_in, "value_in": value_in, "out_saved": out_saved, "out_grad": out_grad, "span_place": span_place}


def reference(query_in, key_in, value_in, out_saved, out_grad, span_place):
    scale = HEAD_DIM ** -0.5
    index = jnp.arange(SEQUENCE_TOKENS, dtype=jnp.int32)
    position = span_place[index // SPAN].astype(jnp.int32) * SPAN + index % SPAN
    visible = position[None, :] <= position[:, None]

    def split_heads(array):
        return array.reshape(SEQUENCE_TOKENS, HEADS, HEAD_DIM).transpose(1, 0, 2)

    delta_all = jnp.sum((out_grad.astype(jnp.float32) * out_saved.astype(jnp.float32)).reshape(SEQUENCE_TOKENS, HEADS, HEAD_DIM), axis=2).T

    def one_head(operands):
        query_head, key_head, value_head, grad_head, delta_head = operands
        scores = jnp.dot(query_head, key_head.T, preferred_element_type=jnp.float32) * scale
        masked = jnp.where(visible, scores, -jnp.inf)
        top = jnp.max(masked, axis=1, keepdims=True)
        lse = top + jnp.log(jnp.sum(jnp.exp(masked - top), axis=1, keepdims=True))
        probs = jnp.exp(jnp.where(visible, scores - lse, -jnp.inf))
        dprobs = jnp.dot(grad_head, value_head.T, preferred_element_type=jnp.float32)
        dscores = (probs * (dprobs - delta_head[:, None]) * scale).astype(jnp.bfloat16)
        grad_q = jnp.dot(dscores, key_head, preferred_element_type=jnp.float32).astype(jnp.bfloat16)
        grad_k = jnp.dot(dscores.T, query_head, preferred_element_type=jnp.float32).astype(jnp.bfloat16)
        grad_v = jnp.dot(probs.astype(jnp.bfloat16).T, grad_head, preferred_element_type=jnp.float32).astype(jnp.bfloat16)
        return grad_q, grad_k, grad_v

    grads = lax.map(one_head, (split_heads(query_in), split_heads(key_in), split_heads(value_in), split_heads(out_grad), delta_all))

    def join_heads(array):
        return array.transpose(1, 0, 2).reshape(SEQUENCE_TOKENS, HEADS * HEAD_DIM)

    return join_heads(grads[0]), join_heads(grads[1]), join_heads(grads[2])
```

```python
import jax
import jax.numpy as jnp
from jax import lax
from jax.experimental import pallas as pl
from jax.experimental.pallas import tpu as pltpu
from jax.sharding import Mesh
from jax.sharding import PartitionSpec as P

HEAD_DIM = 128
SCALE = HEAD_DIM ** (-0.5)
SPAN = 64
HEADS_AXES = ("z", "xh", "c")
KV_AXES = ("yl", "xl", "c")
Q_AXES = ("yh",)
CTX_HEAD = ("yh", "yl", "xl", "c", "z", "xh")
CTX = ("yh", "yl", "xl", "c")
HEAD = ("z", "xh")
NEG = -1e30


def key_positions(place_ref, out_ref):
    first = lax.axis_index("yh") * 16
    row = lax.broadcasted_iota(jnp.int32, (SPAN, HEAD_DIM), 0)
    for s in range(16):
        out_ref[s * SPAN : (s + 1) * SPAN, :] = row + place_ref[first + s] * SPAN


def query_positions(place_ref, b):
    chip = (b * 2 + lax.axis_index("yl")) * 2 + lax.axis_index("xl")
    lane = lax.broadcasted_iota(jnp.int32, (1, 256), 1)
    core_one = ((lane // 8) % 2) == 1
    late = lane >= 128
    at = [[place_ref[chip * 4 + c * 2 + k] for k in range(2)] for c in range(2)]
    place = jnp.where(
        core_one,
        jnp.where(late, at[1][1], at[1][0]),
        jnp.where(late, at[0][1], at[0][0]),
    )
    return place * SPAN + ((lane // 16) % 8) * 8 + lane % 8


def rows_of(ref, b, k):
    return ref[b, :, k].astype(jnp.float32).reshape(256, HEAD_DIM).astype(jnp.bfloat16)


def dot(a, b, dims):
    return lax.dot_general(a, b, (dims, ((), ())), preferred_element_type=jnp.float32)


def stats_kernel(place_ref, own_ref, q_ref, kv_ref, out_ref, kpos_ref):
    key_positions(place_ref, kpos_ref)
    grad = own_ref[:, 1].astype(jnp.float32).reshape(256, HEAD_DIM)
    saved = own_ref[:, 2].astype(jnp.float32).reshape(256, HEAD_DIM)
    delta = jnp.sum((grad * saved).T, axis=0, keepdims=True)
    keys = kv_ref[:, :128].reshape(1024, HEAD_DIM)
    kpos = jnp.concatenate([kpos_ref[...]] * 2, axis=1)
    zeros = jnp.zeros((6, HEAD_DIM), jnp.float32)
    tops, totals = [], []
    for b in range(4):
        scores = dot(keys, rows_of(q_ref, b, 0), ((1,), (1,))) * SCALE
        scores = jnp.where(kpos <= query_positions(place_ref, b), scores, -jnp.inf)
        top = jnp.maximum(jnp.max(scores, axis=0, keepdims=True), NEG)
        total = jnp.sum(jnp.exp(scores - top), axis=0, keepdims=True)
        for k in range(2):
            tops.append(top[:, k * 128 : (k + 1) * 128])
            totals.append(total[:, k * 128 : (k + 1) * 128])
    block = jnp.concatenate(
        tops + totals + [delta[:, :128], delta[:, 128:], zeros], axis=0
    )
    for p in range(4):
        out_ref[p] = block


def grads_kernel(place_ref, stats_ref, q_ref, kv_ref, dq_ref, dkv_ref, kpos_ref, acc_ref):
    key_positions(place_ref, kpos_ref)
    top = jnp.max(stats_ref[:, 0:8], axis=0)
    total = jnp.zeros((8, HEAD_DIM), jnp.float32)
    for p in range(4):
        total += stats_ref[p, 8:16] * jnp.exp(stats_ref[p, 0:8] - top)
    lse8 = top + jnp.log(total)
    lse = jnp.concatenate([lse8[j : j + 1] for j in range(8)], axis=1)
    delta = jnp.concatenate(
        [stats_ref[b, 16 + k : 17 + k] for b in range(4) for k in range(2)], axis=1
    )
    qpos = jnp.concatenate([query_positions(place_ref, b) for b in range(4)], axis=1)
    queries = jnp.concatenate([rows_of(q_ref, b, 0) for b in range(4)], axis=0)
    grads = jnp.concatenate([rows_of(q_ref, b, 1) for b in range(4)], axis=0)
    for j in range(8):
        keys = kv_ref[j, :128]
        values = kv_ref[j, 128:]
        kpos = jnp.concatenate([kpos_ref[j * 128 : (j + 1) * 128, :]] * 8, axis=1)
        scores = dot(keys, queries, ((1,), (1,))) * SCALE
        probs = jnp.exp(jnp.where(kpos <= qpos, scores - lse, -jnp.inf))
        dprobs = dot(values, grads, ((1,), (1,)))
        dscores = (probs * (dprobs - delta) * SCALE).astype(jnp.bfloat16)
        dkv_ref[j, :128] = dot(dscores, queries, ((1,), (0,))).astype(jnp.bfloat16)
        dkv_ref[j, 128:] = dot(probs.astype(jnp.bfloat16), grads, ((1,), (0,))).astype(jnp.bfloat16)
        part = dot(keys.T, dscores, ((1,), (0,)))
        if j == 0:
            acc_ref[...] = part
        else:
            acc_ref[...] += part
    for b in range(4):
        dq_ref[b] = acc_ref[:, b * 256 : (b + 1) * 256].T.astype(jnp.bfloat16)


def kv_pack_kernel(key_ref, value_ref, out_ref):
    for c in range(2):
        block = jnp.concatenate(
            [key_ref[:, c * 128 : (c + 1) * 128], value_ref[:, c * 128 : (c + 1) * 128]], axis=0
        )
        for p in range(4):
            out_ref[p * 2 + c] = block


def q_pack_kernel(own_ref, out_ref):
    block = own_ref[:, :2]
    for p in range(4):
        out_ref[p] = block


def dq_sum_kernel(parts_ref, out_ref):
    total = parts_ref[0].astype(jnp.float32)
    for p in range(1, 4):
        total += parts_ref[p].astype(jnp.float32)
    out_ref[...] = total.astype(jnp.bfloat16)


def dkv_sum_kernel(parts_ref, dk_ref, dv_ref):
    for c in range(2):
        total = parts_ref[c].astype(jnp.float32)
        for p in range(1, 4):
            total += parts_ref[p * 2 + c].astype(jnp.float32)
        total = total.astype(jnp.bfloat16)
        dk_ref[:, c * 128 : (c + 1) * 128] = total[:128]
        dv_ref[:, c * 128 : (c + 1) * 128] = total[128:]


VMEM = pl.BlockSpec(memory_space=pltpu.VMEM)
SMEM = pl.BlockSpec(memory_space=pltpu.SMEM)


def head_tiles(x):
    return x.reshape(8, 32, HEAD_DIM).transpose(1, 0, 2)


def body(query_in, key_in, value_in, out_saved, out_grad, span_place):
    mine = jnp.stack([head_tiles(query_in), head_tiles(out_grad), head_tiles(out_saved)], axis=1)
    own = lax.all_to_all(mine, HEADS_AXES, 0, 0, tiled=True)
    q_send = pl.pallas_call(
        q_pack_kernel,
        out_shape=jax.ShapeDtypeStruct((4, 32, 2, 8, HEAD_DIM), jnp.bfloat16),
        in_specs=[VMEM],
        out_specs=VMEM,
        name="q_pack",
    )(own)
    q_all = lax.all_to_all(q_send, Q_AXES, 0, 0, tiled=True)

    kv_send = pl.pallas_call(
        kv_pack_kernel,
        out_shape=jax.ShapeDtypeStruct((8, 256, HEAD_DIM), jnp.bfloat16),
        in_specs=[VMEM, VMEM],
        out_specs=VMEM,
        name="kv_pack",
    )(key_in, value_in)
    kv_all = lax.all_to_all(kv_send, KV_AXES, 0, 0, tiled=True)

    stats = pl.pallas_call(
        stats_kernel,
        out_shape=jax.ShapeDtypeStruct((4, 24, HEAD_DIM), jnp.float32),
        in_specs=[SMEM, VMEM, VMEM, VMEM],
        out_specs=VMEM,
        scratch_shapes=[pltpu.VMEM((1024, HEAD_DIM), jnp.int32)],
        name="stats",
    )(span_place, own, q_all, kv_all)
    stats_all = lax.all_to_all(stats, Q_AXES, 0, 0, tiled=True)

    dq, dkv = pl.pallas_call(
        grads_kernel,
        out_shape=(
            jax.ShapeDtypeStruct((4, 256, HEAD_DIM), jnp.bfloat16),
            jax.ShapeDtypeStruct((8, 256, HEAD_DIM), jnp.bfloat16),
        ),
        in_specs=[SMEM, VMEM, VMEM, VMEM],
        out_specs=(VMEM, VMEM),
        scratch_shapes=[
            pltpu.VMEM((1024, HEAD_DIM), jnp.int32),
            pltpu.VMEM((HEAD_DIM, 1024), jnp.float32),
        ],
        name="grads",
    )(span_place, stats_all, q_all, kv_all)

    dq_parts = lax.all_to_all(dq, Q_AXES, 0, 0, tiled=True)
    dq_rows = pl.pallas_call(
        dq_sum_kernel,
        out_shape=jax.ShapeDtypeStruct((256, HEAD_DIM), jnp.bfloat16),
        in_specs=[VMEM],
        out_specs=VMEM,
        name="dq_sum",
    )(dq_parts)
    dq_home = lax.all_to_all(dq_rows.reshape(32, 8, HEAD_DIM), HEADS_AXES, 0, 0, tiled=True)
    grad_query = dq_home.transpose(1, 0, 2).reshape(8, 32 * HEAD_DIM)

    dkv_parts = lax.all_to_all(dkv, KV_AXES, 0, 0, tiled=True)
    grad_key, grad_value = pl.pallas_call(
        dkv_sum_kernel,
        out_shape=(jax.ShapeDtypeStruct((128, 256), jnp.bfloat16),) * 2,
        in_specs=[VMEM],
        out_specs=(VMEM, VMEM),
        name="dkv_sum",
    )(dkv_parts)
    return grad_query, grad_key, grad_value


def solution(mesh):
    torus = Mesh(mesh.devices.reshape(4, 2, 2, 2, 8, 2), CTX_HEAD)
    return jax.shard_map(
        body,
        mesh=torus,
        in_specs=(
            P(CTX_HEAD, None),
            P(CTX, HEAD),
            P(CTX, HEAD),
            P(CTX_HEAD, None),
            P(CTX_HEAD, None),
            P(),
        ),
        out_specs=(P(CTX_HEAD, None), P(CTX, HEAD), P(CTX, HEAD)),
        check_vma=False,
    )
```

```python
import jax
import jax.numpy as jnp
from jax import lax
from jax.experimental import pallas as pl
from jax.experimental.pallas import tpu as pltpu
from jax.sharding import Mesh
from jax.sharding import PartitionSpec as P


HEAD_DIM = 128
SCALE = HEAD_DIM ** (-0.5)
SPAN = 64
HEADS_AXES = ("z", "xh", "c")
Q_AXES = ("yl", "xl")
CTX_HEAD = ("yh", "yl", "xl", "c", "z", "xh")
CTX = ("yh", "yl", "xl", "c")
HEAD = ("z", "xh")
NEG = -1e30


def key_positions(place_ref, out_ref):
    row = lax.broadcasted_iota(jnp.int32, (SPAN, HEAD_DIM), 0)
    c = lax.axis_index("c")
    for p in range(4):
        back = lax.rem(lax.axis_index("yh") + (4 - p), 4)
        chip = (back * 2 + lax.axis_index("yl")) * 2 + lax.axis_index("xl")
        for q in range(2):
            first = chip * 4 + (c if q == 0 else 1 - c) * 2
            for k in range(2):
                at = ((p * 2 + q) * 2 + k) * SPAN
                out_ref[at : at + SPAN, :] = row + place_ref[first + k] * SPAN


def query_positions(place_ref, b):
    chip = lax.axis_index("yh") * 4 + b
    lane = lax.broadcasted_iota(jnp.int32, (1, 256), 1)
    core_one = ((lane // 8) % 2) == 1
    late = lane >= 128
    at = [[place_ref[chip * 4 + c * 2 + k] for k in range(2)] for c in range(2)]
    place = jnp.where(
        core_one,
        jnp.where(late, at[1][1], at[1][0]),
        jnp.where(late, at[0][1], at[0][0]),
    )
    return place * SPAN + ((lane // 16) % 8) * 8 + lane % 8


def rows_of(ref, b, k):
    return ref[b, :, k].astype(jnp.float32).reshape(256, HEAD_DIM).astype(jnp.bfloat16)


def dot(a, b, dims):
    return lax.dot_general(a, b, (dims, ((), ())), preferred_element_type=jnp.float32)


def stats_kernel(place_ref, own_ref, q_ref, kv0, kv1, kv2, kv3, out_ref, kpos_ref):
    key_positions(place_ref, kpos_ref)
    grad = own_ref[:, 1].astype(jnp.float32).reshape(256, HEAD_DIM)
    saved = own_ref[:, 2].astype(jnp.float32).reshape(256, HEAD_DIM)
    delta = jnp.sum((grad * saved).T, axis=0, keepdims=True)
    keys = jnp.concatenate(
        [kv[:, :128].reshape(256, HEAD_DIM) for kv in (kv0, kv1, kv2, kv3)], axis=0
    )
    kpos = jnp.concatenate([kpos_ref[...]] * 2, axis=1)
    zeros = jnp.zeros((6, HEAD_DIM), jnp.float32)
    tops, totals = [], []
    for b in range(4):
        scores = dot(keys, rows_of(q_ref, b, 0), ((1,), (1,))) * SCALE
        scores = jnp.where(kpos <= query_positions(place_ref, b), scores, -jnp.inf)
        top = jnp.maximum(jnp.max(scores, axis=0, keepdims=True), NEG)
        total = jnp.sum(jnp.exp(scores - top), axis=0, keepdims=True)
        for k in range(2):
            tops.append(top[:, k * 128 : (k + 1) * 128])
            totals.append(total[:, k * 128 : (k + 1) * 128])
    block = jnp.concatenate(
        tops + totals + [delta[:, :128], delta[:, 128:], zeros], axis=0
    )
    for p in range(4):
        out_ref[p] = block


def grads_kernel(
    place_ref, stats_ref, q_ref, kv0, kv1, kv2, kv3, dq_ref, d0, d1, d2, d3, kpos_ref, acc_ref
):
    key_positions(place_ref, kpos_ref)
    top = jnp.max(stats_ref[:, 0:8], axis=0)
    total = jnp.zeros((8, HEAD_DIM), jnp.float32)
    for p in range(4):
        total += stats_ref[p, 8:16] * jnp.exp(stats_ref[p, 0:8] - top)
    lse8 = top + jnp.log(total)
    lse = jnp.concatenate([lse8[j : j + 1] for j in range(8)], axis=1)
    delta = jnp.concatenate(
        [stats_ref[b, 16 + k : 17 + k] for b in range(4) for k in range(2)], axis=1
    )
    qpos = jnp.concatenate([query_positions(place_ref, b) for b in range(4)], axis=1)
    queries = jnp.concatenate([rows_of(q_ref, b, 0) for b in range(4)], axis=0)
    grads = jnp.concatenate([rows_of(q_ref, b, 1) for b in range(4)], axis=0)
    for j in range(8):
        kv_ref = (kv0, kv1, kv2, kv3)[j // 2]
        dkv_ref = (d0, d1, d2, d3)[j // 2]
        keys = kv_ref[j % 2, :128]
        values = kv_ref[j % 2, 128:]
        kpos = jnp.concatenate([kpos_ref[j * 128 : (j + 1) * 128, :]] * 8, axis=1)
        scores = dot(keys, queries, ((1,), (1,))) * SCALE
        probs = jnp.exp(jnp.where(kpos <= qpos, scores - lse, -jnp.inf))
        dprobs = dot(values, grads, ((1,), (1,)))
        dscores = (probs * (dprobs - delta) * SCALE).astype(jnp.bfloat16)
        dkv_ref[j % 2, :128] = dot(dscores, queries, ((1,), (0,))).astype(jnp.bfloat16)
        dkv_ref[j % 2, 128:] = dot(probs.astype(jnp.bfloat16), grads, ((1,), (0,))).astype(jnp.bfloat16)
        part = dot(keys.T, dscores, ((1,), (0,)))
        if j == 0:
            acc_ref[...] = part
        else:
            acc_ref[...] += part
    for b in range(4):
        dq_ref[b] = acc_ref[:, b * 256 : (b + 1) * 256].T.astype(jnp.bfloat16)


def half(ref, c):
    return ref[:, pl.ds(pl.multiple_of(c * HEAD_DIM, HEAD_DIM), HEAD_DIM)]


def kv_pack_kernel(key_ref, value_ref, keep_ref, give_ref):
    c = lax.axis_index("c")
    keep_ref[:128] = half(key_ref, c)
    keep_ref[128:] = half(value_ref, c)
    give_ref[:128] = half(key_ref, 1 - c)
    give_ref[128:] = half(value_ref, 1 - c)


def join_kernel(keep_ref, got_ref, out_ref):
    out_ref[0] = keep_ref[...]
    out_ref[1] = got_ref[...]


def q_pack_kernel(own_ref, out_ref):
    block = own_ref[:, :2]
    for p in range(4):
        out_ref[p] = block


def dq_sum_kernel(parts_ref, out_ref):
    total = parts_ref[0].astype(jnp.float32)
    for p in range(1, 4):
        total += parts_ref[p].astype(jnp.float32)
    out_ref[...] = total.astype(jnp.bfloat16)


def dkv_sum_kernel(p0, p1, p2, p3, keep_ref, give_ref):
    for q, out_ref in enumerate((keep_ref, give_ref)):
        total = p0[q].astype(jnp.float32)
        for part in (p1, p2, p3):
            total += part[q].astype(jnp.float32)
        out_ref[...] = total.astype(jnp.bfloat16)


def dkv_place_kernel(keep_ref, got_ref, dk_ref, dv_ref):
    c = lax.axis_index("c")
    for ref, at in ((keep_ref, c), (got_ref, 1 - c)):
        columns = pl.ds(pl.multiple_of(at * HEAD_DIM, HEAD_DIM), HEAD_DIM)
        dk_ref[:, columns] = ref[:128]
        dv_ref[:, columns] = ref[128:]


VMEM = pl.BlockSpec(memory_space=pltpu.VMEM)
SMEM = pl.BlockSpec(memory_space=pltpu.SMEM)


def kernel_call(kernel, *, out_shape, in_specs, **options):
    shapes = [pltpu.VMEM(s.shape, s.dtype) for s in jax.tree.leaves(out_shape)]
    call = pl.pallas_call(
        kernel,
        in_specs=in_specs,
        out_shape=shapes[0] if len(shapes) == 1 else tuple(shapes),
        compiler_params=pltpu.CompilerParams(vmem_limit_bytes=32 * 1024 * 1024),
        **options,
    )

    def run(*arrays):
        placed = [
            pltpu.with_memory_space_constraint(a, pltpu.VMEM) if spec is VMEM else a
            for a, spec in zip(arrays, in_specs)
        ]
        return call(*placed)

    return run


def head_tiles(x):
    return x.reshape(8, 32, HEAD_DIM).transpose(1, 0, 2)


def exchange(x, axes):
    return lax.all_to_all(x, axes, 0, 0, tiled=True)


def shift(x, axis, by):
    n = lax.axis_size(axis)
    return lax.ppermute(x, axis, [(i, (i + by) % n) for i in range(n)])


def bf16(*shape):
    return jax.ShapeDtypeStruct(shape, jnp.bfloat16)


def body(query_in, key_in, value_in, out_saved, out_grad, span_place):
    keep, give = kernel_call(
        kv_pack_kernel,
        out_shape=(bf16(256, HEAD_DIM),) * 2,
        in_specs=[VMEM, VMEM],
        out_specs=(VMEM, VMEM),
    )(key_in, value_in)
    got = shift(give, "c", 1)
    kv = kernel_call(
        join_kernel,
        out_shape=bf16(2, 256, HEAD_DIM),
        in_specs=[VMEM, VMEM],
        out_specs=VMEM,
    )(keep, got)
    kvs = [kv] + [shift(kv, "yh", k) for k in (1, 2, 3)]

    mine = jnp.stack([head_tiles(query_in), head_tiles(out_grad), head_tiles(out_saved)], axis=1)
    own = exchange(mine, HEADS_AXES)
    q_send = kernel_call(
        q_pack_kernel,
        out_shape=bf16(4, 32, 2, 8, HEAD_DIM),
        in_specs=[VMEM],
        out_specs=VMEM,
    )(own)
    q_all = exchange(q_send, Q_AXES)

    stats = kernel_call(
        stats_kernel,
        out_shape=jax.ShapeDtypeStruct((4, 24, HEAD_DIM), jnp.float32),
        in_specs=[SMEM] + [VMEM] * 6,
        out_specs=VMEM,
        scratch_shapes=[pltpu.VMEM((1024, HEAD_DIM), jnp.int32)],
    )(span_place, own, q_all, *kvs)
    stats_all = exchange(stats, Q_AXES)

    dq, *dkvs = kernel_call(
        grads_kernel,
        out_shape=(bf16(4, 256, HEAD_DIM),) + (bf16(2, 256, HEAD_DIM),) * 4,
        in_specs=[SMEM] + [VMEM] * 6,
        out_specs=(VMEM,) * 5,
        scratch_shapes=[
            pltpu.VMEM((1024, HEAD_DIM), jnp.int32),
            pltpu.VMEM((HEAD_DIM, 1024), jnp.float32),
        ],
    )(span_place, stats_all, q_all, *kvs)

    parts = [dkvs[0]] + [shift(dkvs[k], "yh", -k) for k in (1, 2, 3)]
    dq_parts = exchange(dq, Q_AXES)
    dq_rows = kernel_call(
        dq_sum_kernel, out_shape=bf16(256, HEAD_DIM), in_specs=[VMEM], out_specs=VMEM
    )(dq_parts)
    dq_home = exchange(dq_rows.reshape(32, 8, HEAD_DIM), HEADS_AXES)
    grad_query = dq_home.transpose(1, 0, 2).reshape(8, 32 * HEAD_DIM)

    keep, give = kernel_call(
        dkv_sum_kernel,
        out_shape=(bf16(256, HEAD_DIM),) * 2,
        in_specs=[VMEM] * 4,
        out_specs=(VMEM, VMEM),
    )(*parts)
    got = shift(give, "c", 1)
    grad_key, grad_value = kernel_call(
        dkv_place_kernel,
        out_shape=(bf16(128, 256),) * 2,
        in_specs=[VMEM, VMEM],
        out_specs=(VMEM, VMEM),
    )(keep, got)
    return grad_query, grad_key, grad_value


def solution(mesh):
    torus = Mesh(mesh.devices.reshape(4, 2, 2, 2, 8, 2), CTX_HEAD)
    return jax.shard_map(
        body,
        mesh=torus,
        in_specs=(
            P(CTX_HEAD, None),
            P(CTX, HEAD),
            P(CTX, HEAD),
            P(CTX_HEAD, None),
            P(CTX_HEAD, None),
            P(),
        ),
        out_specs=(P(CTX_HEAD, None), P(CTX, HEAD), P(CTX, HEAD)),
        check_vma=False,
    )
```

```python
import jax
import jax.numpy as jnp
from jax import lax
from jax.experimental import pallas as pl
from jax.experimental.pallas import tpu as pltpu
from jax.sharding import Mesh
from jax.sharding import PartitionSpec as P


HEAD_DIM = 128
SCALE = HEAD_DIM ** (-0.5)
SPAN = 64
HEADS_AXES = ("z", "xh", "c")
Q_AXES = ("yl", "xl")
CTX_HEAD = ("yh", "yl", "xl", "c", "z", "xh")
CTX = ("yh", "yl", "xl", "c")
HEAD = ("z", "xh")
NEG = -1e30


def key_positions(place_ref, out_ref):
    row = lax.broadcasted_iota(jnp.int32, (SPAN, HEAD_DIM), 0)
    c = lax.axis_index("c")
    for p in range(4):
        back = lax.rem(lax.axis_index("yh") + (4 - p), 4)
        chip = (back * 2 + lax.axis_index("yl")) * 2 + lax.axis_index("xl")
        for q in range(2):
            first = chip * 4 + (c if q == 0 else 1 - c) * 2
            for k in range(2):
                at = ((p * 2 + q) * 2 + k) * SPAN
                out_ref[at : at + SPAN, :] = row + place_ref[first + k] * SPAN


def query_positions(place_ref, b):
    chip = lax.axis_index("yh") * 4 + b
    lane = lax.broadcasted_iota(jnp.int32, (1, 256), 1)
    core_one = ((lane // 8) % 2) == 1
    late = lane >= 128
    at = [[place_ref[chip * 4 + c * 2 + k] for k in range(2)] for c in range(2)]
    place = jnp.where(
        core_one,
        jnp.where(late, at[1][1], at[1][0]),
        jnp.where(late, at[0][1], at[0][0]),
    )
    return place * SPAN + ((lane // 16) % 8) * 8 + lane % 8


def rows_of(ref, b, k):
    return ref[b, :, k].astype(jnp.float32).reshape(256, HEAD_DIM).astype(jnp.bfloat16)


def dot(a, b, dims):
    return lax.dot_general(a, b, (dims, ((), ())), preferred_element_type=jnp.float32)


def stats_kernel(place_ref, own_ref, q_ref, kv0, kv1, kv2, kv3, out_ref, kpos_ref):
    key_positions(place_ref, kpos_ref)
    grad = own_ref[:, 1].astype(jnp.float32).reshape(256, HEAD_DIM)
    saved = own_ref[:, 2].astype(jnp.float32).reshape(256, HEAD_DIM)
    delta = jnp.sum((grad * saved).T, axis=0, keepdims=True)
    keys = jnp.concatenate(
        [kv[:, :128].reshape(256, HEAD_DIM) for kv in (kv0, kv1, kv2, kv3)], axis=0
    )
    kpos = jnp.concatenate([kpos_ref[...]] * 2, axis=1)
    zeros = jnp.zeros((6, HEAD_DIM), jnp.float32)
    tops, totals = [], []
    for b in range(4):
        scores = dot(keys, rows_of(q_ref, b, 0), ((1,), (1,))) * SCALE
        scores = jnp.where(kpos <= query_positions(place_ref, b), scores, -jnp.inf)
        top = jnp.maximum(jnp.max(scores, axis=0, keepdims=True), NEG)
        total = jnp.sum(jnp.exp(scores - top), axis=0, keepdims=True)
        for k in range(2):
            tops.append(top[:, k * 128 : (k + 1) * 128])
            totals.append(total[:, k * 128 : (k + 1) * 128])
    block = jnp.concatenate(
        tops + totals + [delta[:, :128], delta[:, 128:], zeros], axis=0
    )
    for p in range(4):
        out_ref[p] = block


def block_rows(kv_refs, first, count, k):
    at = slice(k * 128, (k + 1) * 128)
    return jnp.concatenate([kv_refs[j // 2][j % 2, at] for j in range(first, first + count)], axis=0)


def grads_kernel(
    place_ref, stats_ref, q_ref, kv0, kv1, kv2, kv3, dq_ref, d0, d1, d2, d3, kpos_ref, acc_ref
):
    key_positions(place_ref, kpos_ref)
    top = jnp.max(stats_ref[:, 0:8], axis=0)
    total = jnp.zeros((8, HEAD_DIM), jnp.float32)
    for p in range(4):
        total += stats_ref[p, 8:16] * jnp.exp(stats_ref[p, 0:8] - top)
    lse8 = top + jnp.log(total)
    lse = jnp.concatenate([lse8[j : j + 1] for j in range(8)], axis=1)
    delta = jnp.concatenate(
        [stats_ref[b, 16 + k : 17 + k] for b in range(4) for k in range(2)], axis=1
    )
    qpos = jnp.concatenate([query_positions(place_ref, b) for b in range(4)], axis=1)
    queries = jnp.concatenate([rows_of(q_ref, b, 0) for b in range(4)], axis=0)
    grads = jnp.concatenate([rows_of(q_ref, b, 1) for b in range(4)], axis=0)
    step = 4
    for first in range(0, 8, step):
        keys = block_rows((kv0, kv1, kv2, kv3), first, step, 0)
        values = block_rows((kv0, kv1, kv2, kv3), first, step, 1)
        kpos = kpos_ref[first * 128 : (first + step) * 128, :]
        kpos = jnp.concatenate([kpos] * 8, axis=1)
        scores = dot(keys, queries, ((1,), (1,))) * SCALE
        probs = jnp.exp(jnp.where(kpos <= qpos, scores - lse, -jnp.inf))
        dprobs = dot(values, grads, ((1,), (1,)))
        dscores = (probs * (dprobs - delta) * SCALE).astype(jnp.bfloat16)
        dk = dot(dscores, queries, ((1,), (0,))).astype(jnp.bfloat16)
        dv = dot(probs.astype(jnp.bfloat16), grads, ((1,), (0,))).astype(jnp.bfloat16)
        for i in range(step):
            d_ref = (d0, d1, d2, d3)[(first + i) // 2]
            d_ref[i % 2, :128] = dk[i * 128 : (i + 1) * 128]
            d_ref[i % 2, 128:] = dv[i * 128 : (i + 1) * 128]
        part = dot(keys.T, dscores, ((1,), (0,)))
        if first == 0:
            acc_ref[...] = part
        else:
            acc_ref[...] += part
    for b in range(4):
        dq_ref[b] = acc_ref[:, b * 256 : (b + 1) * 256].T.astype(jnp.bfloat16)


def half(ref, c):
    return ref[:, pl.ds(pl.multiple_of(c * HEAD_DIM, HEAD_DIM), HEAD_DIM)]


def kv_pack_kernel(key_ref, value_ref, keep_ref, give_ref):
    c = lax.axis_index("c")
    keep_ref[:128] = half(key_ref, c)
    keep_ref[128:] = half(value_ref, c)
    give_ref[:128] = half(key_ref, 1 - c)
    give_ref[128:] = half(value_ref, 1 - c)


def join_kernel(keep_ref, got_ref, out_ref):
    out_ref[0] = keep_ref[...]
    out_ref[1] = got_ref[...]


def q_pack_kernel(own_ref, out_ref):
    block = own_ref[:, :2]
    for p in range(4):
        out_ref[p] = block


def dq_sum_kernel(parts_ref, out_ref):
    total = parts_ref[0].astype(jnp.float32)
    for p in range(1, 4):
        total += parts_ref[p].astype(jnp.float32)
    out_ref[...] = total.astype(jnp.bfloat16)


def dkv_sum_kernel(p0, p1, p2, p3, keep_ref, give_ref):
    for q, out_ref in enumerate((keep_ref, give_ref)):
        total = p0[q].astype(jnp.float32)
        for part in (p1, p2, p3):
            total += part[q].astype(jnp.float32)
        out_ref[...] = total.astype(jnp.bfloat16)


def dkv_place_kernel(keep_ref, got_ref, dk_ref, dv_ref):
    c = lax.axis_index("c")
    for ref, at in ((keep_ref, c), (got_ref, 1 - c)):
        columns = pl.ds(pl.multiple_of(at * HEAD_DIM, HEAD_DIM), HEAD_DIM)
        dk_ref[:, columns] = ref[:128]
        dv_ref[:, columns] = ref[128:]


VMEM = pl.BlockSpec(memory_space=pltpu.VMEM)
SMEM = pl.BlockSpec(memory_space=pltpu.SMEM)


def kernel_call(kernel, *, out_shape, in_specs, final=False, **options):
    shapes = [pltpu.VMEM(s.shape, s.dtype) for s in jax.tree.leaves(out_shape)]
    call = pl.pallas_call(
        kernel,
        in_specs=in_specs,
        out_shape=out_shape if final else shapes[0] if len(shapes) == 1 else tuple(shapes),
        compiler_params=pltpu.CompilerParams(vmem_limit_bytes=32 * 1024 * 1024),
        **options,
    )

    def run(*arrays):
        placed = [
            pltpu.with_memory_space_constraint(a, pltpu.VMEM) if spec is VMEM else a
            for a, spec in zip(arrays, in_specs)
        ]
        return call(*placed)

    return run


def head_tiles(x):
    return x.reshape(8, 32, HEAD_DIM).transpose(1, 0, 2)


def exchange(x, axes):
    return lax.all_to_all(x, axes, 0, 0, tiled=True)


def shift(x, axis, by):
    n = lax.axis_size(axis)
    return lax.ppermute(x, axis, [(i, (i + by) % n) for i in range(n)])


def bf16(*shape):
    return jax.ShapeDtypeStruct(shape, jnp.bfloat16)


def body(query_in, key_in, value_in, out_saved, out_grad, span_place):
    keep, give = kernel_call(
        kv_pack_kernel,
        out_shape=(bf16(256, HEAD_DIM),) * 2,
        in_specs=[VMEM, VMEM],
        out_specs=(VMEM, VMEM),
    )(key_in, value_in)
    got = shift(give, "c", 1)
    kv = kernel_call(
        join_kernel, out_shape=bf16(2, 256, HEAD_DIM), in_specs=[VMEM, VMEM], out_specs=VMEM
    )(keep, got)
    kvs = [kv] + [shift(kv, "yh", k) for k in (1, 2, 3)]

    mine = jnp.stack([head_tiles(query_in), head_tiles(out_grad), head_tiles(out_saved)], axis=1)
    own = exchange(mine, HEADS_AXES)
    q_send = kernel_call(
        q_pack_kernel, out_shape=bf16(4, 32, 2, 8, HEAD_DIM), in_specs=[VMEM], out_specs=VMEM
    )(own)
    q_all = exchange(q_send, Q_AXES)

    stats = kernel_call(
        stats_kernel,
        out_shape=jax.ShapeDtypeStruct((4, 24, HEAD_DIM), jnp.float32),
        in_specs=[SMEM] + [VMEM] * 6,
        out_specs=VMEM,
        scratch_shapes=[pltpu.VMEM((1024, HEAD_DIM), jnp.int32)],
    )(span_place, own, q_all, *kvs)
    stats_all = exchange(stats, Q_AXES)

    dq, *dkvs = kernel_call(
        grads_kernel,
        out_shape=(bf16(4, 256, HEAD_DIM),) + (bf16(2, 256, HEAD_DIM),) * 4,
        in_specs=[SMEM] + [VMEM] * 6,
        out_specs=(VMEM,) * 5,
        scratch_shapes=[
            pltpu.VMEM((1024, HEAD_DIM), jnp.int32),
            pltpu.VMEM((HEAD_DIM, 1024), jnp.float32),
        ],
    )(span_place, stats_all, q_all, *kvs)

    parts = [dkvs[0]] + [shift(dkvs[k], "yh", -k) for k in (1, 2, 3)]
    dq_parts = exchange(dq, Q_AXES)
    dq_rows = kernel_call(
        dq_sum_kernel, out_shape=bf16(256, HEAD_DIM), in_specs=[VMEM], out_specs=VMEM
    )(dq_parts)
    dq_home = exchange(dq_rows.reshape(32, 8, HEAD_DIM), HEADS_AXES)
    grad_query = dq_home.transpose(1, 0, 2).reshape(8, 32 * HEAD_DIM)

    keep, give = kernel_call(
        dkv_sum_kernel,
        out_shape=(bf16(256, HEAD_DIM),) * 2,
        in_specs=[VMEM] * 4,
        out_specs=(VMEM, VMEM),
    )(*parts)
    got = shift(give, "c", 1)
    grad_key, grad_value = kernel_call(
        dkv_place_kernel,
        out_shape=(bf16(128, 256),) * 2,
        in_specs=[VMEM, VMEM],
        out_specs=(VMEM, VMEM),
        final=True,
    )(keep, got)
    return grad_query, grad_key, grad_value


def solution(mesh):
    torus = Mesh(mesh.devices.reshape(4, 2, 2, 2, 8, 2), CTX_HEAD)
    return jax.shard_map(
        body,
        mesh=torus,
        in_specs=(
            P(CTX_HEAD, None),
            P(CTX, HEAD),
            P(CTX, HEAD),
            P(CTX_HEAD, None),
            P(CTX_HEAD, None),
            P(),
        ),
        out_specs=(P(CTX_HEAD, None), P(CTX, HEAD), P(CTX, HEAD)),
        check_vma=False,
    )
```

```python
import jax
import jax.numpy as jnp
from jax import lax
from jax.experimental import pallas as pl
from jax.experimental.pallas import tpu as pltpu
from jax.sharding import Mesh
from jax.sharding import PartitionSpec as P


HEAD_DIM = 128
SCALE = HEAD_DIM ** (-0.5)
SPAN = 64
HEADS_AXES = ("z", "xh", "c")
Q_AXES = ("yl", "xl")
CTX_HEAD = ("yh", "yl", "xl", "c", "z", "xh")
CTX = ("yh", "yl", "xl", "c")
HEAD = ("z", "xh")
NEG = -1e30


def key_positions(place_ref, out_ref):
    row = lax.broadcasted_iota(jnp.int32, (SPAN, HEAD_DIM), 0)
    c = lax.axis_index("c")
    for p in range(4):
        back = lax.axis_index("yh") ^ p
        chip = (back * 2 + lax.axis_index("yl")) * 2 + lax.axis_index("xl")
        for q in range(2):
            first = chip * 4 + (c if q == 0 else 1 - c) * 2
            for k in range(2):
                at = ((p * 2 + q) * 2 + k) * SPAN
                out_ref[at : at + SPAN, :] = row + place_ref[first + k] * SPAN


def query_positions(place_ref, b):
    chip = lax.axis_index("yh") * 4 + b
    lane = lax.broadcasted_iota(jnp.int32, (1, 256), 1)
    core_one = ((lane // 8) % 2) == 1
    late = lane >= 128
    at = [[place_ref[chip * 4 + c * 2 + k] for k in range(2)] for c in range(2)]
    place = jnp.where(
        core_one,
        jnp.where(late, at[1][1], at[1][0]),
        jnp.where(late, at[0][1], at[0][0]),
    )
    return place * SPAN + ((lane // 16) % 8) * 8 + lane % 8


def rows_of(ref, b, k):
    return ref[b, :, k].astype(jnp.float32).reshape(256, HEAD_DIM).astype(jnp.bfloat16)


def dot(a, b, dims):
    return lax.dot_general(a, b, (dims, ((), ())), preferred_element_type=jnp.float32)


def stats_kernel(place_ref, own_ref, q_ref, kv0, kv1, kv2, kv3, out_ref, kpos_ref):
    key_positions(place_ref, kpos_ref)
    grad = own_ref[:, 1].astype(jnp.float32).reshape(256, HEAD_DIM)
    saved = own_ref[:, 2].astype(jnp.float32).reshape(256, HEAD_DIM)
    delta = jnp.sum((grad * saved).T, axis=0, keepdims=True)
    keys = jnp.concatenate(
        [kv[:, :128].reshape(256, HEAD_DIM) for kv in (kv0, kv1, kv2, kv3)], axis=0
    )
    kpos = jnp.concatenate([kpos_ref[...]] * 2, axis=1)
    zeros = jnp.zeros((6, HEAD_DIM), jnp.float32)
    tops, totals = [], []
    for b in range(4):
        scores = dot(keys, rows_of(q_ref, b, 0), ((1,), (1,))) * SCALE
        scores = jnp.where(kpos <= query_positions(place_ref, b), scores, -jnp.inf)
        top = jnp.maximum(jnp.max(scores, axis=0, keepdims=True), NEG)
        total = jnp.sum(jnp.exp(scores - top), axis=0, keepdims=True)
        for k in range(2):
            tops.append(top[:, k * 128 : (k + 1) * 128])
            totals.append(total[:, k * 128 : (k + 1) * 128])
    block = jnp.concatenate(
        tops + totals + [delta[:, :128], delta[:, 128:], zeros], axis=0
    )
    for p in range(4):
        out_ref[p] = block


def block_rows(kv_refs, first, count, k):
    at = slice(k * 128, (k + 1) * 128)
    return jnp.concatenate([kv_refs[j // 2][j % 2, at] for j in range(first, first + count)], axis=0)


def grads_kernel(
    place_ref, stats_ref, q_ref, kv0, kv1, kv2, kv3, dq_ref, d0, d1, d2, d3, kpos_ref, acc_ref
):
    key_positions(place_ref, kpos_ref)
    top = jnp.max(stats_ref[:, 0:8], axis=0)
    total = jnp.zeros((8, HEAD_DIM), jnp.float32)
    for p in range(4):
        total += stats_ref[p, 8:16] * jnp.exp(stats_ref[p, 0:8] - top)
    lse8 = top + jnp.log(total)
    lse = jnp.concatenate([lse8[j : j + 1] for j in range(8)], axis=1)
    delta = jnp.concatenate(
        [stats_ref[b, 16 + k : 17 + k] for b in range(4) for k in range(2)], axis=1
    )
    qpos = jnp.concatenate([query_positions(place_ref, b) for b in range(4)], axis=1)
    queries = jnp.concatenate([rows_of(q_ref, b, 0) for b in range(4)], axis=0)
    grads = jnp.concatenate([rows_of(q_ref, b, 1) for b in range(4)], axis=0)
    step = 4
    for first in range(0, 8, step):
        keys = block_rows((kv0, kv1, kv2, kv3), first, step, 0)
        values = block_rows((kv0, kv1, kv2, kv3), first, step, 1)
        kpos = kpos_ref[first * 128 : (first + step) * 128, :]
        kpos = jnp.concatenate([kpos] * 8, axis=1)
        scores = dot(keys, queries, ((1,), (1,))) * SCALE
        probs = jnp.exp(jnp.where(kpos <= qpos, scores - lse, -jnp.inf))
        dprobs = dot(values, grads, ((1,), (1,)))
        dscores = (probs * (dprobs - delta) * SCALE).astype(jnp.bfloat16)
        dk = dot(dscores, queries, ((1,), (0,))).astype(jnp.bfloat16)
        dv = dot(probs.astype(jnp.bfloat16), grads, ((1,), (0,))).astype(jnp.bfloat16)
        for i in range(step):
            d_ref = (d0, d1, d2, d3)[(first + i) // 2]
            d_ref[i % 2, :128] = dk[i * 128 : (i + 1) * 128]
            d_ref[i % 2, 128:] = dv[i * 128 : (i + 1) * 128]
        part = dot(keys.T, dscores, ((1,), (0,)))
        if first == 0:
            acc_ref[...] = part
        else:
            acc_ref[...] += part
    for b in range(4):
        dq_ref[b] = acc_ref[:, b * 256 : (b + 1) * 256].T.astype(jnp.bfloat16)


def half(ref, c):
    return ref[:, pl.ds(pl.multiple_of(c * HEAD_DIM, HEAD_DIM), HEAD_DIM)]


def kv_pack_kernel(key_ref, value_ref, keep_ref, give_ref):
    c = lax.axis_index("c")
    keep_ref[:128] = half(key_ref, c)
    keep_ref[128:] = half(value_ref, c)
    give_ref[:128] = half(key_ref, 1 - c)
    give_ref[128:] = half(value_ref, 1 - c)


def join_kernel(keep_ref, got_ref, out_ref):
    out_ref[0] = keep_ref[...]
    out_ref[1] = got_ref[...]


def q_pack_kernel(own_ref, out_ref):
    block = own_ref[:, :2]
    for p in range(4):
        out_ref[p] = block


def dq_sum_kernel(parts_ref, out_ref):
    total = parts_ref[0].astype(jnp.float32)
    for p in range(1, 4):
        total += parts_ref[p].astype(jnp.float32)
    out_ref[...] = total.astype(jnp.bfloat16)


def dkv_sum_kernel(p0, p1, p2, p3, keep_ref, give_ref):
    for q, out_ref in enumerate((keep_ref, give_ref)):
        total = p0[q].astype(jnp.float32)
        for part in (p1, p2, p3):
            total += part[q].astype(jnp.float32)
        out_ref[...] = total.astype(jnp.bfloat16)


def dkv_place_kernel(keep_ref, got_ref, dk_ref, dv_ref):
    c = lax.axis_index("c")
    for ref, at in ((keep_ref, c), (got_ref, 1 - c)):
        columns = pl.ds(pl.multiple_of(at * HEAD_DIM, HEAD_DIM), HEAD_DIM)
        dk_ref[:, columns] = ref[:128]
        dv_ref[:, columns] = ref[128:]


VMEM = pl.BlockSpec(memory_space=pltpu.VMEM)
SMEM = pl.BlockSpec(memory_space=pltpu.SMEM)


def kernel_call(kernel, *, out_shape, in_specs, final=False, **options):
    shapes = [pltpu.VMEM(s.shape, s.dtype) for s in jax.tree.leaves(out_shape)]
    call = pl.pallas_call(
        kernel,
        in_specs=in_specs,
        out_shape=out_shape if final else shapes[0] if len(shapes) == 1 else tuple(shapes),
        compiler_params=pltpu.CompilerParams(vmem_limit_bytes=32 * 1024 * 1024),
        **options,
    )

    def run(*arrays):
        placed = [
            pltpu.with_memory_space_constraint(a, pltpu.VMEM) if spec is VMEM else a
            for a, spec in zip(arrays, in_specs)
        ]
        return call(*placed)

    return run


def head_tiles(x):
    return x.reshape(8, 32, HEAD_DIM).transpose(1, 0, 2)


def exchange(x, axes):
    return lax.all_to_all(x, axes, 0, 0, tiled=True)


def swap(x, axis, bits):
    return lax.ppermute(x, axis, [(i, i ^ bits) for i in range(lax.axis_size(axis))])


def bf16(*shape):
    return jax.ShapeDtypeStruct(shape, jnp.bfloat16)


def body(query_in, key_in, value_in, out_saved, out_grad, span_place):
    keep, give = kernel_call(
        kv_pack_kernel,
        out_shape=(bf16(256, HEAD_DIM),) * 2,
        in_specs=[VMEM, VMEM],
        out_specs=(VMEM, VMEM),
    )(key_in, value_in)
    got = swap(give, "c", 1)
    kv = kernel_call(
        join_kernel, out_shape=bf16(2, 256, HEAD_DIM), in_specs=[VMEM, VMEM], out_specs=VMEM
    )(keep, got)
    kvs = [kv] + [swap(kv, "yh", k) for k in (1, 2, 3)]

    mine = jnp.stack([head_tiles(query_in), head_tiles(out_grad), head_tiles(out_saved)], axis=1)
    own = exchange(mine, HEADS_AXES)
    q_send = kernel_call(
        q_pack_kernel, out_shape=bf16(4, 32, 2, 8, HEAD_DIM), in_specs=[VMEM], out_specs=VMEM
    )(own)
    q_all = exchange(q_send, Q_AXES)

    stats = kernel_call(
        stats_kernel,
        out_shape=jax.ShapeDtypeStruct((4, 24, HEAD_DIM), jnp.float32),
        in_specs=[SMEM] + [VMEM] * 6,
        out_specs=VMEM,
        scratch_shapes=[pltpu.VMEM((1024, HEAD_DIM), jnp.int32)],
    )(span_place, own, q_all, *kvs)
    stats_all = exchange(stats, Q_AXES)

    dq, *dkvs = kernel_call(
        grads_kernel,
        out_shape=(bf16(4, 256, HEAD_DIM),) + (bf16(2, 256, HEAD_DIM),) * 4,
        in_specs=[SMEM] + [VMEM] * 6,
        out_specs=(VMEM,) * 5,
        scratch_shapes=[
            pltpu.VMEM((1024, HEAD_DIM), jnp.int32),
            pltpu.VMEM((HEAD_DIM, 1024), jnp.float32),
        ],
    )(span_place, stats_all, q_all, *kvs)

    parts = [dkvs[0]] + [swap(dkvs[k], "yh", k) for k in (1, 2, 3)]
    dq_parts = exchange(dq, Q_AXES)
    dq_rows = kernel_call(
        dq_sum_kernel, out_shape=bf16(256, HEAD_DIM), in_specs=[VMEM], out_specs=VMEM
    )(dq_parts)
    dq_home = exchange(dq_rows.reshape(32, 8, HEAD_DIM), HEADS_AXES)
    grad_query = dq_home.transpose(1, 0, 2).reshape(8, 32 * HEAD_DIM)

    keep, give = kernel_call(
        dkv_sum_kernel,
        out_shape=(bf16(256, HEAD_DIM),) * 2,
        in_specs=[VMEM] * 4,
        out_specs=(VMEM, VMEM),
    )(*parts)
    got = swap(give, "c", 1)
    grad_key, grad_value = kernel_call(
        dkv_place_kernel,
        out_shape=(bf16(128, 256),) * 2,
        in_specs=[VMEM, VMEM],
        out_specs=(VMEM, VMEM),
        final=True,
    )(keep, got)
    return grad_query, grad_key, grad_value


def solution(mesh):
    torus = Mesh(mesh.devices.reshape(4, 2, 2, 2, 8, 2), CTX_HEAD)
    return jax.shard_map(
        body,
        mesh=torus,
        in_specs=(
            P(CTX_HEAD, None),
            P(CTX, HEAD),
            P(CTX, HEAD),
            P(CTX_HEAD, None),
            P(CTX_HEAD, None),
            P(),
        ),
        out_specs=(P(CTX_HEAD, None), P(CTX, HEAD), P(CTX, HEAD)),
        check_vma=False,
    )
```

```python
import jax
import jax.numpy as jnp
from jax import lax
from jax.experimental import pallas as pl
from jax.experimental.pallas import tpu as pltpu
from jax.sharding import Mesh
from jax.sharding import PartitionSpec as P


HEAD_DIM = 128
SCALE = HEAD_DIM ** (-0.5)
LOG2_E = 1.4426950408889634
SPAN = 64
HEADS_AXES = ("z", "xh", "c")
Q_AXES = ("yl", "xl")
CTX_HEAD = ("yh", "yl", "xl", "c", "z", "xh")
CTX = ("yh", "yl", "xl", "c")
HEAD = ("z", "xh")
NEG = -1e30


def key_positions(place_ref, out_ref):
    row = lax.broadcasted_iota(jnp.int32, (SPAN, HEAD_DIM), 0)
    c = lax.axis_index("c")
    for p in range(4):
        back = lax.axis_index("yh") ^ p
        chip = (back * 2 + lax.axis_index("yl")) * 2 + lax.axis_index("xl")
        for q in range(2):
            first = chip * 4 + (c if q == 0 else 1 - c) * 2
            for k in range(2):
                at = ((p * 2 + q) * 2 + k) * SPAN
                out_ref[at : at + SPAN, :] = row + place_ref[first + k] * SPAN


def query_positions(place_ref, b):
    chip = lax.axis_index("yh") * 4 + b
    lane = lax.broadcasted_iota(jnp.int32, (1, 256), 1)
    core_one = ((lane // 8) % 2) == 1
    late = lane >= 128
    at = [[place_ref[chip * 4 + c * 2 + k] for k in range(2)] for c in range(2)]
    place = jnp.where(
        core_one,
        jnp.where(late, at[1][1], at[1][0]),
        jnp.where(late, at[0][1], at[0][0]),
    )
    return place * SPAN + ((lane // 16) % 8) * 8 + lane % 8


def rows_of(ref, b, k):
    return ref[b, :, k].astype(jnp.float32).reshape(256, HEAD_DIM).astype(jnp.bfloat16)


def dot(a, b, dims):
    return lax.dot_general(a, b, (dims, ((), ())), preferred_element_type=jnp.float32)


def stats_kernel(place_ref, own_ref, q_ref, kv0, kv1, kv2, kv3, out_ref, kpos_ref):
    key_positions(place_ref, kpos_ref)
    grad = own_ref[:, 1].astype(jnp.float32).reshape(256, HEAD_DIM)
    saved = own_ref[:, 2].astype(jnp.float32).reshape(256, HEAD_DIM)
    delta = jnp.sum((grad * saved).T, axis=0, keepdims=True)
    keys = jnp.concatenate(
        [kv[:, :128].reshape(256, HEAD_DIM) for kv in (kv0, kv1, kv2, kv3)], axis=0
    )
    kpos = jnp.concatenate([kpos_ref[...]] * 2, axis=1)
    zeros = jnp.zeros((6, HEAD_DIM), jnp.float32)
    tops, totals = [], []
    for b in range(4):
        scores = dot(keys, rows_of(q_ref, b, 0), ((1,), (1,)))
        scores = jnp.where(kpos <= query_positions(place_ref, b), scores, -jnp.inf)
        top = jnp.maximum(jnp.max(scores, axis=0, keepdims=True), NEG) * SCALE
        exps = jnp.exp2(scores * (SCALE * LOG2_E) - top * LOG2_E)
        total = jnp.sum(exps, axis=0, keepdims=True)
        for k in range(2):
            tops.append(top[:, k * 128 : (k + 1) * 128])
            totals.append(total[:, k * 128 : (k + 1) * 128])
    block = jnp.concatenate(
        tops + totals + [delta[:, :128], delta[:, 128:], zeros], axis=0
    )
    for p in range(4):
        out_ref[p] = block


def block_rows(kv_refs, first, count, k):
    at = slice(k * 128, (k + 1) * 128)
    return jnp.concatenate([kv_refs[j // 2][j % 2, at] for j in range(first, first + count)], axis=0)


def grads_kernel(
    place_ref, stats_ref, q_ref, kv0, kv1, kv2, kv3, dq_ref, d0, d1, d2, d3, kpos_ref, acc_ref
):
    key_positions(place_ref, kpos_ref)
    top = jnp.max(stats_ref[:, 0:8], axis=0)
    total = jnp.zeros((8, HEAD_DIM), jnp.float32)
    for p in range(4):
        total += stats_ref[p, 8:16] * jnp.exp(stats_ref[p, 0:8] - top)
    lse8 = (top + jnp.log(total)) * LOG2_E
    lse = jnp.concatenate([lse8[j : j + 1] for j in range(8)], axis=1)
    delta = jnp.concatenate(
        [stats_ref[b, 16 + k : 17 + k] for b in range(4) for k in range(2)], axis=1
    )
    qpos = jnp.concatenate([query_positions(place_ref, b) for b in range(4)], axis=1)
    queries = jnp.concatenate([rows_of(q_ref, b, 0) for b in range(4)], axis=0)
    grads = jnp.concatenate([rows_of(q_ref, b, 1) for b in range(4)], axis=0)
    step = 4
    for first in range(0, 8, step):
        keys = block_rows((kv0, kv1, kv2, kv3), first, step, 0)
        values = block_rows((kv0, kv1, kv2, kv3), first, step, 1)
        kpos = kpos_ref[first * 128 : (first + step) * 128, :]
        kpos = jnp.concatenate([kpos] * 8, axis=1)
        scores = dot(keys, queries, ((1,), (1,))) * (SCALE * LOG2_E) - lse
        probs = jnp.exp2(jnp.where(kpos <= qpos, scores, -jnp.inf))
        dprobs = dot(values, grads, ((1,), (1,)))
        dscores = (probs * (dprobs - delta) * SCALE).astype(jnp.bfloat16)
        dk = dot(dscores, queries, ((1,), (0,))).astype(jnp.bfloat16)
        dv = dot(probs.astype(jnp.bfloat16), grads, ((1,), (0,))).astype(jnp.bfloat16)
        for i in range(step):
            d_ref = (d0, d1, d2, d3)[(first + i) // 2]
            d_ref[i % 2, :128] = dk[i * 128 : (i + 1) * 128]
            d_ref[i % 2, 128:] = dv[i * 128 : (i + 1) * 128]
        part = dot(keys.T, dscores, ((1,), (0,)))
        if first == 0:
            acc_ref[...] = part
        else:
            acc_ref[...] += part
    for b in range(4):
        dq_ref[b] = acc_ref[:, b * 256 : (b + 1) * 256].T.astype(jnp.bfloat16)


def half(ref, c):
    return ref[:, pl.ds(pl.multiple_of(c * HEAD_DIM, HEAD_DIM), HEAD_DIM)]


def kv_pack_kernel(key_ref, value_ref, keep_ref, give_ref):
    c = lax.axis_index("c")
    keep_ref[:128] = half(key_ref, c)
    keep_ref[128:] = half(value_ref, c)
    give_ref[:128] = half(key_ref, 1 - c)
    give_ref[128:] = half(value_ref, 1 - c)


def join_kernel(keep_ref, got_ref, out_ref):
    out_ref[0] = keep_ref[...]
    out_ref[1] = got_ref[...]


def q_pack_kernel(own_ref, out_ref):
    block = own_ref[:, :2]
    for p in range(4):
        out_ref[p] = block


def dq_sum_kernel(parts_ref, out_ref):
    total = parts_ref[0].astype(jnp.float32)
    for p in range(1, 4):
        total += parts_ref[p].astype(jnp.float32)
    out_ref[...] = total.astype(jnp.bfloat16)


def dkv_sum_kernel(p0, p1, p2, p3, keep_ref, give_ref):
    for q, out_ref in enumerate((keep_ref, give_ref)):
        total = p0[q].astype(jnp.float32)
        for part in (p1, p2, p3):
            total += part[q].astype(jnp.float32)
        out_ref[...] = total.astype(jnp.bfloat16)


def dkv_place_kernel(keep_ref, got_ref, dk_ref, dv_ref):
    c = lax.axis_index("c")
    for ref, at in ((keep_ref, c), (got_ref, 1 - c)):
        columns = pl.ds(pl.multiple_of(at * HEAD_DIM, HEAD_DIM), HEAD_DIM)
        dk_ref[:, columns] = ref[:128]
        dv_ref[:, columns] = ref[128:]


VMEM = pl.BlockSpec(memory_space=pltpu.VMEM)
SMEM = pl.BlockSpec(memory_space=pltpu.SMEM)


def kernel_call(kernel, *, out_shape, in_specs, final=False, **options):
    shapes = [pltpu.VMEM(s.shape, s.dtype) for s in jax.tree.leaves(out_shape)]
    call = pl.pallas_call(
        kernel,
        in_specs=in_specs,
        out_shape=out_shape if final else shapes[0] if len(shapes) == 1 else tuple(shapes),
        compiler_params=pltpu.CompilerParams(vmem_limit_bytes=32 * 1024 * 1024),
        **options,
    )

    def run(*arrays):
        placed = [
            pltpu.with_memory_space_constraint(a, pltpu.VMEM) if spec is VMEM else a
            for a, spec in zip(arrays, in_specs)
        ]
        return call(*placed)

    return run


def head_tiles(x):
    return x.reshape(8, 32, HEAD_DIM).transpose(1, 0, 2)


def exchange(x, axes):
    return lax.all_to_all(x, axes, 0, 0, tiled=True)


def swap(x, axis, bits):
    return lax.ppermute(x, axis, [(i, i ^ bits) for i in range(lax.axis_size(axis))])


def bf16(*shape):
    return jax.ShapeDtypeStruct(shape, jnp.bfloat16)


def body(query_in, key_in, value_in, out_saved, out_grad, span_place):
    keep, give = kernel_call(
        kv_pack_kernel,
        out_shape=(bf16(256, HEAD_DIM),) * 2,
        in_specs=[VMEM, VMEM],
        out_specs=(VMEM, VMEM),
    )(key_in, value_in)
    got = swap(give, "c", 1)
    kv = kernel_call(
        join_kernel, out_shape=bf16(2, 256, HEAD_DIM), in_specs=[VMEM, VMEM], out_specs=VMEM
    )(keep, got)
    kvs = [kv] + [swap(kv, "yh", k) for k in (1, 2, 3)]

    mine = jnp.stack([head_tiles(query_in), head_tiles(out_grad), head_tiles(out_saved)], axis=1)
    own = exchange(mine, HEADS_AXES)
    q_send = kernel_call(
        q_pack_kernel, out_shape=bf16(4, 32, 2, 8, HEAD_DIM), in_specs=[VMEM], out_specs=VMEM
    )(own)
    q_all = exchange(q_send, Q_AXES)

    stats = kernel_call(
        stats_kernel,
        out_shape=jax.ShapeDtypeStruct((4, 24, HEAD_DIM), jnp.float32),
        in_specs=[SMEM] + [VMEM] * 6,
        out_specs=VMEM,
        scratch_shapes=[pltpu.VMEM((1024, HEAD_DIM), jnp.int32)],
    )(span_place, own, q_all, *kvs)
    stats_all = exchange(stats, Q_AXES)

    dq, *dkvs = kernel_call(
        grads_kernel,
        out_shape=(bf16(4, 256, HEAD_DIM),) + (bf16(2, 256, HEAD_DIM),) * 4,
        in_specs=[SMEM] + [VMEM] * 6,
        out_specs=(VMEM,) * 5,
        scratch_shapes=[
            pltpu.VMEM((1024, HEAD_DIM), jnp.int32),
            pltpu.VMEM((HEAD_DIM, 1024), jnp.float32),
        ],
    )(span_place, stats_all, q_all, *kvs)

    parts = [dkvs[0]] + [swap(dkvs[k], "yh", k) for k in (1, 2, 3)]
    dq_parts = exchange(dq, Q_AXES)
    dq_rows = kernel_call(
        dq_sum_kernel, out_shape=bf16(256, HEAD_DIM), in_specs=[VMEM], out_specs=VMEM
    )(dq_parts)
    dq_home = exchange(dq_rows.reshape(32, 8, HEAD_DIM), HEADS_AXES)
    grad_query = dq_home.transpose(1, 0, 2).reshape(8, 32 * HEAD_DIM)

    keep, give = kernel_call(
        dkv_sum_kernel,
        out_shape=(bf16(256, HEAD_DIM),) * 2,
        in_specs=[VMEM] * 4,
        out_specs=(VMEM, VMEM),
    )(*parts)
    got = swap(give, "c", 1)
    grad_key, grad_value = kernel_call(
        dkv_place_kernel,
        out_shape=(bf16(128, 256),) * 2,
        in_specs=[VMEM, VMEM],
        out_specs=(VMEM, VMEM),
        final=True,
    )(keep, got)
    return grad_query, grad_key, grad_value


def solution(mesh):
    torus = Mesh(mesh.devices.reshape(4, 2, 2, 2, 8, 2), CTX_HEAD)
    return jax.shard_map(
        body,
        mesh=torus,
        in_specs=(
            P(CTX_HEAD, None),
            P(CTX, HEAD),
            P(CTX, HEAD),
            P(CTX_HEAD, None),
            P(CTX_HEAD, None),
            P(),
        ),
        out_specs=(P(CTX_HEAD, None), P(CTX, HEAD), P(CTX, HEAD)),
        check_vma=False,
    )
```
